32 devices in a mesh: rows: 4 (over z), tp: 4 (over y, x), unit: 2 (over core).
Axes of the slice: x: 2, y: 2, z: 4, core: 2. Of those that a mesh axis runs over, the one named last changes fastest.
Arguments:
- train_query: bfloat16 [4096, 2048], P(('unit', 'rows'), 'tp'), parts along dimension 0, may hold values from -0.125 to 0.125
- low_query: bfloat16 [4096, 64], P(('unit', 'rows')), parts along dimension 0, may hold values from -0.125 to 0.125
- high_query: bfloat16 [128, 2048], P('unit', 'tp'), parts along dimension 0, may hold values from -0.75 to 0.75
- train_key: bfloat16 [4096, 512], P(('unit', 'rows'), 'tp'), parts along dimension 0, may hold values from -0.125 to 0.125
- low_key: bfloat16 [4096, 64], P(('unit', 'rows')), parts along dimension 0, may hold values from -0.125 to 0.125
- high_key: bfloat16 [128, 512], P('unit', 'tp'), parts along dimension 0, may hold values from -0.75 to 0.75
- train_value: bfloat16 [4096, 512], P(('unit', 'rows'), 'tp'), parts along dimension 0, may hold values from -0.125 to 0.125
- low_value: bfloat16 [4096, 64], P(('unit', 'rows')), parts along dimension 0, may hold values from -0.125 to 0.125
- high_value: bfloat16 [128, 512], P('unit', 'tp'), parts along dimension 0, may hold values from -0.75 to 0.75
- norm_train: float32 [4096], P(('unit', 'rows', 'tp')), parts along dimension 0, may hold values from 0.25 to 1.75
- norm_step: float32 [4096], P(('unit', 'rows', 'tp')), parts along dimension 0, may hold values from -0.3 to 0.3
Outputs:
- final_query: bfloat16 [4096, 2048], P(('unit', 'tp')), parts along dimension 0
- final_key: bfloat16 [1024, 2048], P(('unit', 'tp')), parts along dimension 0
- final_value: bfloat16 [1024, 2048], P(('unit', 'tp')), parts along dimension 0
- serve_norm: bfloat16 [4096], P('unit'), parts along dimension 0
The draws below stay inside these ranges and needn't reach their ends.
There are 2 independent parts, one for each index of `unit`. The reference program is written for one: setup_inputs(seed, part) draws one part's arguments, and reference() takes and returns one part's arrays. A program takes and returns all parts, laid end to end along the dimension named above; each array names one. Nothing has to cross between parts.
All inputs are finite; a program needn't handle non-finite values.
Results may differ from the reference program's by a relative error of at most 0.001.
Values may be sent and summed in bfloat16 or wider, within the bound.
A program may use at most 64 MiB of HBM per device.

```python
import jax
import jax.numpy as jnp

D_MODEL = 2048
Q_DIM = 2048
KV_DIM = 512
RANK = 64


def block_levels(key, dims, split, least, largest):
    def one(axis_at, blocks):
        heights = jax.random.uniform(jax.random.fold_in(jax.random.fold_in(key, 6), axis_at), (blocks,), jnp.float32, least / len(split), largest / len(split))
        return jnp.repeat(jnp.exp(heights), dims[axis_at] // blocks).reshape((-1,) + (1,) * (len(dims) - axis_at - 1))

    gain = one(*split[0])
    for cut in split[1:]:
        gain = gain * one(*cut)
    return gain


def scatter_about(key, shape, scale, bound, cuts=(), kind=jnp.bfloat16):
    result = jax.random.normal(key, shape, jnp.float32) * scale
    if len(cuts) > 0:
        result = block_levels(key, shape, cuts, -0.22, 0.18) * result
    return jnp.clip(result, min=-bound, max=bound).astype(kind)


def setup_inputs(seed: int = 0, part: int = 0) -> dict:
    streams_of = jax.random.split(jax.random.key(seed), 12)
    own_keys = jax.random.split(jax.random.fold_in(streams_of[11], part), 12)
    return {
        "train_query": scatter_about(own_keys[0], (D_MODEL, Q_DIM), D_MODEL ** -0.5, 0.125, ((0, 4), (1, 4))),
        "low_query": scatter_about(own_keys[1], (D_MODEL, RANK), D_MODEL ** -0.5, 0.125, ((0, 4),)),
        "high_query": scatter_about(own_keys[2], (RANK, Q_DIM), RANK ** -0.5, 0.75, ((1, 4),)),
        "train_key": scatter_about(own_keys[3], (D_MODEL, KV_DIM), D_MODEL ** -0.5, 0.125, ((0, 4), (1, 4))),
        "low_key": scatter_about(own_keys[4], (D_MODEL, RANK), D_MODEL ** -0.5, 0.125, ((0, 4),)),
        "high_key": scatter_about(own_keys[5], (RANK, KV_DIM), RANK ** -0.5, 0.75, ((1, 4),)),
        "train_value": scatter_about(own_keys[6], (D_MODEL, KV_DIM), D_MODEL ** -0.5, 0.125, ((0, 4), (1, 4))),
        "low_value": scatter_about(own_keys[7], (D_MODEL, RANK), D_MODEL ** -0.5, 0.125, ((0, 4),)),
        "high_value": scatter_about(own_keys[8], (RANK, KV_DIM), RANK ** -0.5, 0.75, ((1, 4),)),
        "norm_train": jnp.clip(1.0 + 0.15 * jax.random.normal(own_keys[9], (D_MODEL,), jnp.float32), 0.25, 1.75),
        "norm_step": jnp.clip(jax.random.uniform(own_keys[10], (D_MODEL,), jnp.float32, -0.3, 0.3) * block_levels(own_keys[10], (D_MODEL,), ((0, 16),), -0.4, 0.0), -0.3, 0.3),
    }


mix_rate = 0.5


def reference(train_query, low_query, high_query, train_key, low_key, high_key, train_value, low_value, high_value, norm_train, norm_step):
    result_query = train_query.astype(jnp.float32) + mix_rate * jnp.dot(low_query, high_query, preferred_element_type=jnp.float32)
    result_key = train_key.astype(jnp.float32) + mix_rate * jnp.dot(low_key, high_key, preferred_element_type=jnp.float32)
    result_value = train_value.astype(jnp.float32) + mix_rate * jnp.dot(low_value, high_value, preferred_element_type=jnp.float32)
    final_query = result_query.T.astype(jnp.bfloat16)
    final_key = result_key.T.astype(jnp.bfloat16)
    final_value = result_value.T.astype(jnp.bfloat16)
    serve_norm = (norm_train + norm_step).astype(jnp.bfloat16)
    return final_query, final_key, final_value, serve_norm
```

```python
import functools

import jax
import jax.numpy as jnp
from jax import lax
from jax.experimental import pallas as pl
from jax.experimental.pallas import tpu as pltpu
from jax.sharding import PartitionSpec as P

mix_rate = 0.5
MESH = pl.DeviceIdType.MESH
LANES = 128
ORDER = (1, 2, 0)


def plan(heights):
    units, row = [], 0
    for which in ORDER:
        height = heights[which]
        width = LANES if height % LANES == 0 else height
        for start in range(0, height, width):
            units.append((which, start, width, row))
            row += width
    edges = [unit[3] for unit in units] + [row]
    cuts = sorted({0, 1, 1 + -(-3 * (len(units) - 1) // 5), len(units)})
    spans = [(a, b, edges[a], edges[b] - edges[a]) for a, b in zip(cuts, cuts[1:])]
    return units, spans, row


def partners(peers, part):
    if peers & (peers - 1):
        return [[(lax.rem(part + step, peers), part, 1) for step in range(1, peers)]]
    rounds, size = [], 1
    while size < peers:
        low = lax.rem(part, 2 * size) < size
        rounds.append([(jnp.where(low, part + size, part - size), part - lax.rem(part, size), size)])
        size *= 2
    return rounds


def kernel(n, peers, rows, units, spans, *refs):
    (tq, lq, hq, tk, lk, hk, tv, lv, hv, norm_train, norm_step) = refs[:11]
    gathered, out_norm = refs[11:13]
    held = refs[13:24]
    (gains, sums, in_sem, send_sem, recv_sem, peer_send, peer_recv, ready) = refs[24:]
    me, part = lax.axis_index("rows"), lax.axis_index("tp")
    right, left = lax.rem(me + 1, n), lax.rem(me + n - 1, n)
    has_right, has_left = me < n - 1, me > 0
    rounds = partners(peers, part)
    greeted = sum(len(group) for group in rounds)

    barrier = pltpu.get_barrier_semaphore()

    def greet(axis, index):
        pl.semaphore_signal(barrier, inc=1, device_id={axis: index}, device_id_type=MESH)

    loads = [
        pltpu.make_async_copy(source, target, in_sem.at[i])
        for i, (source, target) in enumerate(zip(refs[:11], held))
    ]

    @pl.when(has_right)
    def _():
        greet("rows", right)

    for group in rounds:
        for whom, _, _ in group:
            greet("tp", whom)
    for which in ORDER:
        for i in (1, 2, 0):
            loads[3 * which + i].start()
        if which == ORDER[0]:
            loads[9].start()
            loads[10].start()

    last = len(spans)
    norm_piece = last - 1

    def view(c, k):
        if c == norm_piece:
            return gains.at[k]
        _, _, start, height = spans[min(c, last - 1)]
        if len(gathered.shape) == 3:
            return gathered.at[k, pl.ds(start, height), :]
        return gathered.at[pl.ds(start, height), pl.ds(pl.multiple_of(k * rows, rows), rows)]

    def hop(c, k, way):
        return pltpu.make_async_remote_copy(
            src_ref=view(c, k),
            dst_ref=view(c, k),
            send_sem=send_sem.at[way, k, c],
            recv_sem=recv_sem.at[k, c],
            device_id={"rows": left if way else right},
            device_id_type=MESH,
        )

    def send(c, way):
        @pl.when(has_left if way else has_right)
        def _():
            hop(c, me, way).start()

    loaded = set()

    def merge(u):
        which, start, width, row = units[u]
        train, low, high = held[3 * which : 3 * which + 3]
        if which not in loaded:
            loaded.add(which)
            for i in (1, 2, 0):
                loads[3 * which + i].wait()
        span = pl.ds(start, width)
        product = lax.dot_general(
            high[:, span], low[...], (((0,), (0,)), ((), ())), preferred_element_type=jnp.float32
        )
        result = train[:, span].T.astype(jnp.float32) + mix_rate * product
        if len(gathered.shape) == 3:
            target = gathered.at[me, pl.ds(row, width), :]
        else:
            target = gathered.at[pl.ds(row, width), pl.ds(pl.multiple_of(me * rows, rows), rows)]
        target[...] = result.astype(jnp.bfloat16)

    def merge_span(c):
        for u in range(spans[min(c, last - 1)][0], spans[min(c, last - 1)][1]):
            merge(u)

    bulk = [c for c in range(last + 1) if c != norm_piece]
    merge_span(bulk[0])
    loads[9].wait()
    loads[10].wait()
    gains[me, part] = held[9][...] + held[10][...]
    pl.semaphore_wait(barrier, greeted + has_left.astype(jnp.int32))

    @pl.when(has_left)
    def _():
        pl.semaphore_signal(ready, inc=1, device_id={"rows": left}, device_id_type=MESH)

    send(bulk[0], 1)
    for c in bulk[1:]:
        merge_span(c)
        if c < norm_piece:
            send(c, 1)

    @pl.when(has_right)
    def _():
        pl.semaphore_wait(ready, 1)

    for c in bulk:
        if c < norm_piece:
            send(c, 0)

    flight = 0
    for group in rounds:
        copies = []
        for whom, first, size in group:
            entries = gains.at[me, pl.ds(first, size)]
            copies.append(
                pltpu.make_async_remote_copy(
                    src_ref=entries,
                    dst_ref=entries,
                    send_sem=peer_send.at[flight],
                    recv_sem=peer_recv.at[flight],
                    device_id={"tp": whom},
                    device_id_type=MESH,
                )
            )
            flight += 1
        for copy in copies:
            copy.start()
        for copy in copies:
            copy.wait()
    for way in (1, 0):
        for c in (norm_piece, last):
            send(c, way)

    def pass_on(step, carry):
        for c in range(last + 1):

            @pl.when(me + step < n)
            def _():
                hop(c, me + step, 1).wait_recv()

                @pl.when(has_left)
                def _():
                    hop(c, me + step, 1).start()

            @pl.when(me - step >= 0)
            def _():
                hop(c, me - step, 0).wait_recv()

                @pl.when(has_right)
                def _():
                    hop(c, me - step, 0).start()

        return carry

    lax.fori_loop(1, n - 1, pass_on, 0)

    def arrive(c):
        if n > 1:

            @pl.when(me == 0)
            def _():
                hop(c, n - 1, 1).wait_recv()

            @pl.when(me == n - 1)
            def _():
                hop(c, 0, 0).wait_recv()

    for c in range(last):
        arrive(c)
    for k in range(n):
        for t in range(peers):
            sums[k * peers + t : k * peers + t + 1, :] = gains[k, t]
    out_norm[...] = sums[...].astype(jnp.bfloat16)

    def sent(step, carry):
        for c in range(last + 1):

            @pl.when((me - step >= 0) & has_right)
            def _():
                hop(c, me - step, 0).wait_send()

            @pl.when((me + step < n) & has_left)
            def _():
                hop(c, me + step, 1).wait_send()

        return carry

    lax.fori_loop(0, n, sent, 0)
    arrive(last)


def settle(places, gathered, norm, *refs):
    *outs, out_norm, sem = refs
    copies = [
        pltpu.make_async_copy(gathered.at[pl.ds(row, out.shape[0]), :], out, sem.at[i])
        for i, (row, out) in enumerate(zip(places, outs))
    ]
    copies.append(pltpu.make_async_copy(norm, out_norm, sem.at[len(outs)]))
    for copy in copies:
        copy.start()
    for copy in copies:
        copy.wait()


def solution(mesh):
    n, peers = mesh.shape["rows"], mesh.shape["tp"]

    def shards(tq, lq, hq, tk, lk, hk, tv, lv, hv, norm_train, norm_step):
        rows = tq.shape[0]
        whole_tiles = rows % LANES == 0
        operands = (
            tq, lq.T, hq, tk, lk.T, hk, tv, lv.T, hv,
            norm_train.reshape(1, -1), norm_step.reshape(1, -1),
        )
        heights = [train.shape[1] for train in (tq, tk, tv)]
        units, spans, total = plan(heights)
        places = [min(row for which, _, _, row in units if which == i) for i in range(3)]
        width = norm_train.shape[0]
        place = pltpu.VMEM if whole_tiles else jax.ShapeDtypeStruct
        shape = (total, n * rows) if whole_tiles else (n, total, rows)
        flights = max(1, peers - 1)
        gathered, norm = pl.pallas_call(
            functools.partial(kernel, n, peers, rows, units, spans),
            out_shape=[
                place(shape, jnp.bfloat16),
                place((n * peers, width), jnp.bfloat16),
            ],
            in_specs=[pl.BlockSpec(memory_space=pl.ANY)] * len(operands),
            out_specs=[pl.BlockSpec(memory_space=pltpu.VMEM)] * 2,
            scratch_shapes=[pltpu.VMEM(x.shape, x.dtype) for x in operands]
            + [
                pltpu.VMEM((n, peers, 1, width), jnp.float32),
                pltpu.VMEM((n * peers, width), jnp.float32),
                pltpu.SemaphoreType.DMA((len(operands),)),
                pltpu.SemaphoreType.DMA((2, n, len(spans) + 1)),
                pltpu.SemaphoreType.DMA((n, len(spans) + 1)),
                pltpu.SemaphoreType.DMA((flights,)),
                pltpu.SemaphoreType.DMA((flights,)),
                pltpu.SemaphoreType.REGULAR,
            ],
            compiler_params=pltpu.CompilerParams(collective_id=0, has_side_effects=True),
        )(*operands)
        if whole_tiles:
            *finals, norm = pl.pallas_call(
                functools.partial(settle, places),
                out_shape=[
                    jax.ShapeDtypeStruct((height, n * rows), jnp.bfloat16) for height in heights
                ]
                + [jax.ShapeDtypeStruct(norm.shape, norm.dtype)],
                in_specs=[pl.BlockSpec(memory_space=pltpu.VMEM)] * 2,
                out_specs=[pl.BlockSpec(memory_space=pl.ANY)] * 4,
                scratch_shapes=[pltpu.SemaphoreType.DMA((4,))],
                compiler_params=pltpu.CompilerParams(vmem_limit_bytes=8 * 1024 * 1024),
            )(gathered, norm)
            return (*finals, norm.reshape(-1))
        finals = [
            gathered[:, row : row + height, :].transpose(1, 0, 2).reshape(height, n * rows)
            for row, height in zip(places, heights)
        ]
        return (*finals, norm.reshape(-1))

    in_specs = (
        P(("unit", "rows"), "tp"),
        P(("unit", "rows"), None),
        P("unit", "tp"),
    ) * 3 + (P(("unit", "rows", "tp")),) * 2
    out_specs = (P(("unit", "tp"), None),) * 3 + (P("unit"),)
    return jax.shard_map(shards, mesh=mesh, in_specs=in_specs, out_specs=out_specs, check_vma=False)
```

```python
import functools

import jax
import jax.numpy as jnp
from jax import lax
from jax.experimental import pallas as pl
from jax.experimental.pallas import tpu as pltpu
from jax.sharding import PartitionSpec as P

mix_rate = 0.5
MESH = pl.DeviceIdType.MESH
LANES = 128
ORDER = (1, 2, 0)


def plan(heights):
    units, row = [], 0
    for which in ORDER:
        height = heights[which]
        width = LANES if height % LANES == 0 else height
        for start in range(0, height, width):
            units.append((which, start, width, row))
            row += width
    edges = [unit[3] for unit in units] + [row]
    cut = sum(unit[0] != ORDER[-1] for unit in units)
    spans = [(0, cut, 0, edges[cut]), (cut, len(units), edges[cut], row - edges[cut])]
    return units, spans, row


def partners(peers, part):
    if peers & (peers - 1):
        return [[(lax.rem(part + step, peers), part, 1) for step in range(1, peers)]]
    rounds, size = [], 1
    while size < peers:
        low = lax.rem(part, 2 * size) < size
        rounds.append([(jnp.where(low, part + size, part - size), part - lax.rem(part, size), size)])
        size *= 2
    return rounds


def kernel(n, peers, rows, early, units, spans, *refs):
    (tq, lq, hq, tk, lk, hk, tv, lv, hv, norm_train, norm_step) = refs[:11]
    gathered, out_norm = refs[11:13]
    held = refs[13:24]
    (gains, sums, raw_train, raw_low) = refs[24:28]
    (in_sem, send_sem, recv_sem, raw_sem, peer_send, peer_recv, signs) = refs[28:]
    me, part, unit = lax.axis_index("rows"), lax.axis_index("tp"), lax.axis_index("unit")
    right, left = lax.rem(me + 1, n), lax.rem(me + n - 1, n)
    has_right, has_left = me < n - 1, me > 0
    rounds = partners(peers, part)
    flat = [whom for group in rounds for whom, _, _ in group]
    told, known = 1, 1 + len(flat)

    barrier = pltpu.get_barrier_semaphore()

    def sign(sem, axis, index):
        pl.semaphore_signal(sem, inc=1, device_id={axis: index}, device_id_type=MESH)

    loads = [
        pltpu.make_async_copy(source, target, in_sem.at[i])
        for i, (source, target) in enumerate(zip(refs[:11], held))
    ]

    @pl.when(has_right)
    def _():
        sign(barrier, "rows", right)

    @pl.when(me == 0)
    def _():
        for whom in flat:
            sign(barrier, "tp", whom)

    for which in ORDER[:2]:
        for i in (1, 2, 0):
            loads[3 * which + i].start()
    pl.semaphore_wait(barrier, jnp.where(has_left, 1, len(flat)))

    @pl.when(has_left)
    def _():
        sign(signs.at[0], "rows", left)

    raws = [
        pltpu.make_async_remote_copy(
            src_ref=source,
            dst_ref=target,
            send_sem=raw_sem.at[i],
            recv_sem=raw_sem.at[2 + i],
            device_id={"rows": left},
            device_id_type=MESH,
        )
        for i, (source, target) in enumerate(
            [(tq.at[pl.ds(0, LANES), :], raw_train), (lq.at[:, pl.ds(0, LANES)], raw_low)]
            if early
            else []
        )
    ]

    @pl.when(me == 1)
    def _():
        for raw in raws:
            raw.start()

    for i in (1, 2, 0, 9, 10):
        loads[i].start()

    FIRST, GAINS, SECOND = range(3)

    def view(c, k, trimmed=False):
        if c == GAINS:
            return gains.at[k]
        _, _, start, height = spans[c // 2]
        if len(gathered.shape) == 3:
            return gathered.at[k, pl.ds(start, height), :]
        skip = LANES if trimmed else 0
        column = pl.multiple_of(k * rows + skip, LANES)
        return gathered.at[pl.ds(start, height), pl.ds(column, rows - skip)]

    def hop(c, k, way, trimmed=False):
        slot = k - 1 if way else k
        return pltpu.make_async_remote_copy(
            src_ref=view(c, k, trimmed),
            dst_ref=view(c, k, trimmed),
            send_sem=send_sem.at[way, k, c],
            recv_sem=recv_sem.at[slot, c],
            device_id={"rows": left if way else right},
            device_id_type=MESH,
        )

    def send(c, way):
        if not way:

            @pl.when(has_right)
            def _():
                hop(c, me, 0).start()

        elif early and c == SECOND:

            @pl.when(me == 1)
            def _():
                hop(c, me, 1, True).start()

            @pl.when(me > 1)
            def _():
                hop(c, me, 1).start()

        else:

            @pl.when(has_left)
            def _():
                hop(c, me, 1).start()

    loaded = set()

    def put(row, width, k, skip, count, high, low, train):
        product = lax.dot_general(
            high, low, (((0,), (0,)), ((), ())), preferred_element_type=jnp.float32
        )
        result = train.T.astype(jnp.float32) + mix_rate * product
        if len(gathered.shape) == 3:
            target = gathered.at[k, pl.ds(row, width), :]
        else:
            column = pl.multiple_of(k * rows + skip, LANES)
            target = gathered.at[pl.ds(row, width), pl.ds(column, count)]
        target[...] = result.astype(jnp.bfloat16)

    def merge(u):
        which, start, width, row = units[u]
        train, low, high = held[3 * which : 3 * which + 3]
        if which not in loaded:
            loaded.add(which)
            for i in (1, 2, 0):
                loads[3 * which + i].wait()
        span = pl.ds(start, width)
        put(row, width, me, 0, rows, high[:, span], low[...], train[:, span])

    def merge_span(c):
        for u in range(*spans[c // 2][:2]):
            merge(u)

    merge_span(FIRST)
    send(FIRST, 1)

    @pl.when(has_right)
    def _():
        pl.semaphore_wait(signs.at[0], 1)

    send(FIRST, 0)
    merge_span(SECOND)

    def send_second():
        send(SECOND, 1)
        send(SECOND, 0)

    @pl.when(unit == 0)
    def _():
        send_second()

    loads[9].wait()
    loads[10].wait()
    gains[me, part] = held[9][...] + held[10][...]

    @pl.when(has_left)
    def _():
        for j in range(len(flat)):
            pl.semaphore_wait(signs.at[known + j], 1)

    @pl.when(has_right)
    def _():
        for j, whom in enumerate(flat):
            sign(signs.at[told + j], "tp", whom)
        for j in range(len(flat)):
            pl.semaphore_wait(signs.at[told + j], 1)
            sign(signs.at[known + j], "rows", right)

    flight = 0
    for group in rounds:
        copies = []
        for whom, first, size in group:
            entries = gains.at[me, pl.ds(first, size)]
            copies.append(
                pltpu.make_async_remote_copy(
                    src_ref=entries,
                    dst_ref=entries,
                    send_sem=peer_send.at[flight],
                    recv_sem=peer_recv.at[flight],
                    device_id={"tp": whom},
                    device_id_type=MESH,
                )
            )
            flight += 1
        for copy in copies:
            copy.start()
        for copy in copies:
            copy.wait()
    @pl.when(unit != 0)
    def _():
        send_second()

    send(GAINS, 1)
    send(GAINS, 0)

    def take_left(c, step):
        if early and c == SECOND and isinstance(step, int) and step == 1:

            @pl.when(me == 0)
            def _():
                hop(c, me + step, 1, True).wait_recv()

            @pl.when(me > 0)
            def _():
                hop(c, me + step, 1).wait_recv()

        else:
            hop(c, me + step, 1).wait_recv()

    def pass_on(step, carry):
        for c in range(3):

            @pl.when(me + step < n)
            def _():
                take_left(c, step)

                @pl.when(has_left)
                def _():
                    hop(c, me + step, 1).start()

            @pl.when(me - step >= 0)
            def _():
                hop(c, me - step, 0).wait_recv()

                @pl.when(has_right)
                def _():
                    hop(c, me - step, 0).start()

        return carry

    def arrive(c):
        if n > 1:

            @pl.when(me == 0)
            def _():
                take_left(c, n - 1)

            @pl.when(me == n - 1)
            def _():
                hop(c, 0, 0).wait_recv()

    if n > 2:
        pass_on(1, 0)
        lax.fori_loop(2, n - 1, pass_on, 0)

    @pl.when(me == 0)
    def _():
        for raw in raws:
            raw.wait_recv()
        for which, start, width, row in units if raws else []:
            if which == 0:
                span = pl.ds(start, width)
                put(row, width, 1, 0, LANES, held[2][:, span], raw_low[...], raw_train[:, span])

    arrive(FIRST)
    arrive(GAINS)
    for k in range(n):
        for t in range(peers):
            sums[k * peers + t : k * peers + t + 1, :] = gains[k, t]
    out_norm[...] = sums[...].astype(jnp.bfloat16)

    @pl.when(me == 1)
    def _():
        for raw in raws:
            raw.wait_send()

    def sent_left(c, step):
        if early and c == SECOND and isinstance(step, int) and step == 0:

            @pl.when(me == 1)
            def _():
                hop(c, me + step, 1, True).wait_send()

            @pl.when(me > 1)
            def _():
                hop(c, me + step, 1).wait_send()

        else:

            @pl.when(has_left)
            def _():
                hop(c, me + step, 1).wait_send()

    def sent(step, carry):
        for c in range(3):

            @pl.when((me - step >= 0) & has_right)
            def _():
                hop(c, me - step, 0).wait_send()

            @pl.when(me + step < n)
            def _():
                sent_left(c, step)

        return carry

    sent(0, 0)
    lax.fori_loop(1, n, sent, 0)
    arrive(SECOND)


def settle(places, gathered, norm, *refs):
    *outs, out_norm, sem = refs
    copies = [
        pltpu.make_async_copy(gathered.at[pl.ds(row, out.shape[0]), :], out, sem.at[i])
        for i, (row, out) in enumerate(zip(places, outs))
    ]
    copies.append(pltpu.make_async_copy(norm, out_norm, sem.at[len(outs)]))
    for copy in copies:
        copy.start()
    for copy in copies:
        copy.wait()


def solution(mesh):
    n, peers = mesh.shape["rows"], mesh.shape["tp"]

    def shards(tq, lq, hq, tk, lk, hk, tv, lv, hv, norm_train, norm_step):
        rows = tq.shape[0]
        whole_tiles = rows % LANES == 0
        operands = (
            tq, lq.T, hq, tk, lk.T, hk, tv, lv.T, hv,
            norm_train.reshape(1, -1), norm_step.reshape(1, -1),
        )
        heights = [train.shape[1] for train in (tq, tk, tv)]
        units, spans, total = plan(heights)
        places = [min(row for which, _, _, row in units if which == i) for i in range(3)]
        width = norm_train.shape[0]
        place = pltpu.VMEM if whole_tiles else jax.ShapeDtypeStruct
        shape = (total, n * rows) if whole_tiles else (n, total, rows)
        rounds = partners(peers, 0)
        flights = max(1, sum(len(group) for group in rounds))
        early = n > 1 and whole_tiles and rows > LANES and heights[0] % LANES == 0
        raw = LANES if early else rows
        gathered, norm = pl.pallas_call(
            functools.partial(kernel, n, peers, rows, early, units, spans),
            out_shape=[
                place(shape, jnp.bfloat16),
                place((n * peers, width), jnp.bfloat16),
            ],
            in_specs=[pl.BlockSpec(memory_space=pl.ANY)] * len(operands),
            out_specs=[pl.BlockSpec(memory_space=pltpu.VMEM)] * 2,
            scratch_shapes=[pltpu.VMEM(x.shape, x.dtype) for x in operands]
            + [
                pltpu.VMEM((n, peers, 1, width), jnp.float32),
                pltpu.VMEM((n * peers, width), jnp.float32),
                pltpu.VMEM((raw, tq.shape[1]), tq.dtype),
                pltpu.VMEM((lq.shape[1], raw), lq.dtype),
                pltpu.SemaphoreType.DMA((len(operands),)),
                pltpu.SemaphoreType.DMA((2, n, 3)),
                pltpu.SemaphoreType.DMA((max(1, n - 1), 3)),
                pltpu.SemaphoreType.DMA((4,)),
                pltpu.SemaphoreType.DMA((flights,)),
                pltpu.SemaphoreType.DMA((flights,)),
                pltpu.SemaphoreType.REGULAR((1 + 2 * flights,)),
            ],
            compiler_params=pltpu.CompilerParams(collective_id=0, has_side_effects=True),
        )(*operands)
        if whole_tiles:
            *finals, norm = pl.pallas_call(
                functools.partial(settle, places),
                out_shape=[
                    jax.ShapeDtypeStruct((height, n * rows), jnp.bfloat16) for height in heights
                ]
                + [jax.ShapeDtypeStruct(norm.shape, norm.dtype)],
                in_specs=[pl.BlockSpec(memory_space=pltpu.VMEM)] * 2,
                out_specs=[pl.BlockSpec(memory_space=pl.ANY)] * 4,
                scratch_shapes=[pltpu.SemaphoreType.DMA((4,))],
                compiler_params=pltpu.CompilerParams(vmem_limit_bytes=8 * 1024 * 1024),
            )(gathered, norm)
            return (*finals, norm.reshape(-1))
        finals = [
            gathered[:, row : row + height, :].transpose(1, 0, 2).reshape(height, n * rows)
            for row, height in zip(places, heights)
        ]
        return (*finals, norm.reshape(-1))

    in_specs = (
        P(("unit", "rows"), "tp"),
        P(("unit", "rows"), None),
        P("unit", "tp"),
    ) * 3 + (P(("unit", "rows", "tp")),) * 2
    out_specs = (P(("unit", "tp"), None),) * 3 + (P("unit"),)
    return jax.shard_map(shards, mesh=mesh, in_specs=in_specs, out_specs=out_specs, check_vma=False)
```

```python
import functools

import jax
import jax.numpy as jnp
from jax import lax
from jax.experimental import pallas as pl
from jax.experimental.pallas import tpu as pltpu
from jax.sharding import PartitionSpec as P

mix_rate = 0.5
MESH = pl.DeviceIdType.MESH
LANES, SUBLANES = 128, 16
ORDER = (1, 2, 0)


def plan(heights):
    units, row = [], 0
    for which in ORDER:
        height = heights[which]
        width = LANES if height % LANES == 0 else height
        for start in range(0, height, width):
            units.append((which, start, width, row))
            row += width
    edges = [unit[3] for unit in units] + [row]
    cut = sum(unit[0] != ORDER[-1] for unit in units)
    spans = [(0, cut, 0, edges[cut]), (cut, len(units), edges[cut], row - edges[cut])]
    return units, spans, row


def partners(peers, part):
    if peers & (peers - 1):
        return [[(lax.rem(part + step, peers), part, 1) for step in range(1, peers)]]
    rounds, size = [], 1
    while size < peers:
        low = lax.rem(part, 2 * size) < size
        rounds.append([(jnp.where(low, part + size, part - size), part - lax.rem(part, size), size)])
        size *= 2
    return rounds


def kernel(n, peers, rows, early, units, spans, *refs):
    (tq, lq, hq, tk, lk, hk, tv, lv, hv, norm_train, norm_step) = refs[:11]
    gathered, out_norm = refs[11:13]
    held = refs[13:24]
    (gains, sums, raw_train, raw_low, via) = refs[24:29]
    (in_sem, send_sem, recv_sem, raw_sem, low_sem, share_sem, via_sem) = refs[29:36]
    (peer_send, peer_recv, signs) = refs[36:]
    me, part, unit = lax.axis_index("rows"), lax.axis_index("tp"), lax.axis_index("unit")
    right, left = lax.rem(me + 1, n), lax.rem(me + n - 1, n)
    has_right, has_left = me < n - 1, me > 0
    rounds = partners(peers, part)
    flat = [whom for group in rounds for whom, _, _ in group]
    told, known = 1, 1 + len(flat)

    barrier = pltpu.get_barrier_semaphore()

    def sign(sem, axis, index):
        pl.semaphore_signal(sem, inc=1, device_id={axis: index}, device_id_type=MESH)

    loads = [
        pltpu.make_async_copy(source, target, in_sem.at[i])
        for i, (source, target) in enumerate(zip(refs[:11], held))
    ]

    @pl.when(has_right)
    def _():
        sign(barrier, "rows", right)

    @pl.when(me == 0)
    def _():
        for whom in flat:
            sign(barrier, "tp", whom)

    for which in ORDER[:2]:
        for i in (1, 2, 0):
            loads[3 * which + i].start()
    pl.semaphore_wait(barrier, jnp.where(has_left, 1, len(flat)))

    @pl.when(has_left)
    def _():
        sign(signs.at[0], "rows", left)

    def raw_down():
        return pltpu.make_async_remote_copy(
            src_ref=tq.at[pl.ds(0, raw_train.shape[0]), :],
            dst_ref=raw_train,
            send_sem=raw_sem.at[0],
            recv_sem=raw_sem.at[1],
            device_id={"rows": left},
            device_id_type=MESH,
        )

    half = raw_low.shape[0] // 2
    carriers = (1, 2)

    def low_down(j):
        return pltpu.make_async_remote_copy(
            src_ref=lq.at[pl.ds(j * half, half), pl.ds(0, LANES)],
            dst_ref=raw_low.at[pl.ds(j * half, half), :],
            send_sem=low_sem.at[0],
            recv_sem=low_sem.at[1 + j],
            device_id={"rows": left},
            device_id_type=MESH,
        )

    def low_across(j, step):
        return pltpu.make_async_remote_copy(
            src_ref=raw_low.at[pl.ds(j * half, half), :],
            dst_ref=raw_low.at[pl.ds(j * half, half), :],
            send_sem=share_sem.at[step - 1],
            recv_sem=low_sem.at[1 + j],
            device_id={"tp": lax.rem(carriers[j] + step, peers)},
            device_id_type=MESH,
        )

    def detour(j, leg):
        rows_there = pl.ds(gathered.shape[0] - (2 - j) * SUBLANES, SUBLANES)
        block = gathered.at[rows_there, pl.ds(rows + LANES, rows - LANES)]
        return pltpu.make_async_remote_copy(
            src_ref=(block, via, via)[leg],
            dst_ref=(via, via, block)[leg],
            send_sem=via_sem.at[j],
            recv_sem=via_sem.at[2 + j],
            device_id=({"tp": carriers[j]}, {"rows": left}, {"tp": 0})[leg],
            device_id_type=MESH,
        )

    if early:

        @pl.when(me == 1)
        def _():
            raw_down().start()

            for j in range(2):

                @pl.when(part == carriers[j])
                def _():
                    low_down(j).start()

    for i in (1, 2, 0, 9, 10):
        loads[i].start()

    FIRST, GAINS, SECOND = range(3)

    def view(c, k, trimmed=0):
        if c == GAINS:
            return gains.at[k]
        _, _, start, height = spans[c // 2]
        if len(gathered.shape) == 3:
            return gathered.at[k, pl.ds(start, height), :]
        skip = LANES if trimmed else 0
        height -= 2 * SUBLANES if trimmed == 2 else 0
        column = pl.multiple_of(k * rows + skip, LANES)
        return gathered.at[pl.ds(start, height), pl.ds(column, rows - skip)]

    def hop(c, k, way, trimmed=0):
        slot = k - 1 if way else k
        return pltpu.make_async_remote_copy(
            src_ref=view(c, k, trimmed),
            dst_ref=view(c, k, trimmed),
            send_sem=send_sem.at[way, k, c],
            recv_sem=recv_sem.at[slot, c],
            device_id={"rows": left if way else right},
            device_id_type=MESH,
        )

    def send(c, way):
        if not way:

            @pl.when(has_right)
            def _():
                hop(c, me, 0).start()

        elif early and c == SECOND:

            @pl.when((me == 1) & (part == 0))
            def _():
                hop(c, me, 1, 2).start()

            @pl.when((me == 1) & (part > 0))
            def _():
                hop(c, me, 1, 1).start()

            @pl.when(me > 1)
            def _():
                hop(c, me, 1).start()

        else:

            @pl.when(has_left)
            def _():
                hop(c, me, 1).start()

    loaded = set()

    def put(row, width, k, skip, count, high, low, train):
        product = lax.dot_general(
            high, low, (((0,), (0,)), ((), ())), preferred_element_type=jnp.float32
        )
        result = train.T.astype(jnp.float32) + mix_rate * product
        if len(gathered.shape) == 3:
            target = gathered.at[k, pl.ds(row, width), :]
        else:
            column = pl.multiple_of(k * rows + skip, LANES)
            target = gathered.at[pl.ds(row, width), pl.ds(column, count)]
        target[...] = result.astype(jnp.bfloat16)

    def merge(u):
        which, start, width, row = units[u]
        train, low, high = held[3 * which : 3 * which + 3]
        if which not in loaded:
            loaded.add(which)
            for i in (1, 2, 0):
                loads[3 * which + i].wait()
        span = pl.ds(start, width)
        put(row, width, me, 0, rows, high[:, span], low[...], train[:, span])

    def merge_span(c):
        for u in range(*spans[c // 2][:2]):
            merge(u)

    merge_span(FIRST)
    send(FIRST, 1)

    @pl.when(has_right)
    def _():
        pl.semaphore_wait(signs.at[0], 1)

    send(FIRST, 0)
    merge_span(SECOND)

    def send_second():
        send(SECOND, 1)
        send(SECOND, 0)

    @pl.when(unit == 0)
    def _():
        send_second()

    loads[9].wait()
    loads[10].wait()
    gains[me, part] = held[9][...] + held[10][...]

    @pl.when(has_left)
    def _():
        for j in range(len(flat)):
            pl.semaphore_wait(signs.at[known + j], 1)

    @pl.when(has_right)
    def _():
        for j, whom in enumerate(flat):
            sign(signs.at[told + j], "tp", whom)
        for j in range(len(flat)):
            pl.semaphore_wait(signs.at[told + j], 1)
            sign(signs.at[known + j], "rows", right)

    flight = 0
    for group in rounds:
        copies = []
        for whom, first, size in group:
            entries = gains.at[me, pl.ds(first, size)]
            copies.append(
                pltpu.make_async_remote_copy(
                    src_ref=entries,
                    dst_ref=entries,
                    send_sem=peer_send.at[flight],
                    recv_sem=peer_recv.at[flight],
                    device_id={"tp": whom},
                    device_id_type=MESH,
                )
            )
            flight += 1
        for copy in copies:
            copy.start()
        for copy in copies:
            copy.wait()
    @pl.when(unit != 0)
    def _():
        send_second()

    if early:

        @pl.when(me == 1)
        def _():
            for j in range(2):

                @pl.when(part == 0)
                def _():
                    detour(j, 0).start()

                @pl.when(part == carriers[j])
                def _():
                    detour(j, 0).wait_recv()
                    detour(j, 1).start()

    send(GAINS, 1)
    send(GAINS, 0)

    def take_left(c, step):
        if early and c == SECOND and isinstance(step, int) and step == 1:

            @pl.when((me == 0) & (part == 0))
            def _():
                hop(c, me + step, 1, 2).wait_recv()

            @pl.when((me == 0) & (part > 0))
            def _():
                hop(c, me + step, 1, 1).wait_recv()

            @pl.when(me > 0)
            def _():
                hop(c, me + step, 1).wait_recv()

        else:
            hop(c, me + step, 1).wait_recv()

    def pass_on(step, carry):
        for c in range(3):

            @pl.when(me + step < n)
            def _():
                take_left(c, step)

                @pl.when(has_left)
                def _():
                    hop(c, me + step, 1).start()

            @pl.when(me - step >= 0)
            def _():
                hop(c, me - step, 0).wait_recv()

                @pl.when(has_right)
                def _():
                    hop(c, me - step, 0).start()

        return carry

    def arrive(c):
        if n > 1:

            @pl.when(me == 0)
            def _():
                take_left(c, n - 1)

            @pl.when(me == n - 1)
            def _():
                hop(c, 0, 0).wait_recv()

    def end_of_line():
        for j in range(2):

            @pl.when(part == carriers[j])
            def _():
                low_down(j).wait_recv()
                for step in range(1, peers):
                    low_across(j, step).start()
                detour(j, 1).wait_recv()
                detour(j, 2).start()

        for j in range(2):

            @pl.when(part != carriers[j])
            def _():
                low_across(j, 1).wait_recv()

        raw_down().wait_recv()
        for which, start, width, row in units:
            if which == 0:
                span = pl.ds(start, width)
                put(row, width, 1, 0, LANES, held[2][:, span], raw_low[...], raw_train[:, span])
        for j in range(2):

            @pl.when(part == 0)
            def _():
                detour(j, 2).wait_recv()

            @pl.when(part == carriers[j])
            def _():
                detour(j, 2).wait_send()
                for step in range(1, peers):
                    low_across(j, step).wait_send()

    if n > 2:
        pass_on(1, 0)
    if early:

        @pl.when(me == 0)
        def _():
            end_of_line()

    if n > 2:
        lax.fori_loop(2, n - 1, pass_on, 0)

    arrive(FIRST)
    arrive(GAINS)
    for k in range(n):
        for t in range(peers):
            sums[k * peers + t : k * peers + t + 1, :] = gains[k, t]
    out_norm[...] = sums[...].astype(jnp.bfloat16)

    if early:

        @pl.when(me == 1)
        def _():
            raw_down().wait_send()
            for j in range(2):

                @pl.when(part == 0)
                def _():
                    detour(j, 0).wait_send()

                @pl.when(part == carriers[j])
                def _():
                    low_down(j).wait_send()
                    detour(j, 1).wait_send()

    def sent_left(c, step):
        if early and c == SECOND and isinstance(step, int) and step == 0:

            @pl.when((me == 1) & (part == 0))
            def _():
                hop(c, me + step, 1, 2).wait_send()

            @pl.when((me == 1) & (part > 0))
            def _():
                hop(c, me + step, 1, 1).wait_send()

            @pl.when(me > 1)
            def _():
                hop(c, me + step, 1).wait_send()

        else:

            @pl.when(has_left)
            def _():
                hop(c, me + step, 1).wait_send()

    def sent(step, carry):
        for c in range(3):

            @pl.when((me - step >= 0) & has_right)
            def _():
                hop(c, me - step, 0).wait_send()

            @pl.when(me + step < n)
            def _():
                sent_left(c, step)

        return carry

    sent(0, 0)
    lax.fori_loop(1, n, sent, 0)
    arrive(SECOND)


def settle(places, gathered, norm, *refs):
    *outs, out_norm, sem = refs
    copies = [
        pltpu.make_async_copy(gathered.at[pl.ds(row, out.shape[0]), :], out, sem.at[i])
        for i, (row, out) in enumerate(zip(places, outs))
    ]
    copies.append(pltpu.make_async_copy(norm, out_norm, sem.at[len(outs)]))
    for copy in copies:
        copy.start()
    for copy in copies:
        copy.wait()


def solution(mesh):
    n, peers = mesh.shape["rows"], mesh.shape["tp"]

    def shards(tq, lq, hq, tk, lk, hk, tv, lv, hv, norm_train, norm_step):
        rows = tq.shape[0]
        whole_tiles = rows % LANES == 0
        operands = (
            tq, lq.T, hq, tk, lk.T, hk, tv, lv.T, hv,
            norm_train.reshape(1, -1), norm_step.reshape(1, -1),
        )
        heights = [train.shape[1] for train in (tq, tk, tv)]
        units, spans, total = plan(heights)
        places = [min(row for which, _, _, row in units if which == i) for i in range(3)]
        width = norm_train.shape[0]
        place = pltpu.VMEM if whole_tiles else jax.ShapeDtypeStruct
        shape = (total, n * rows) if whole_tiles else (n, total, rows)
        rounds = partners(peers, 0)
        flights = max(1, sum(len(group) for group in rounds))
        rank = lq.shape[1]
        early = n > 2 and peers > 2 and whole_tiles and rows > LANES
        early = early and heights[0] % LANES == 0 and rank % (2 * SUBLANES) == 0
        raw = LANES if early else rows
        gathered, norm = pl.pallas_call(
            functools.partial(kernel, n, peers, rows, early, units, spans),
            out_shape=[
                place(shape, jnp.bfloat16),
                place((n * peers, width), jnp.bfloat16),
            ],
            in_specs=[pl.BlockSpec(memory_space=pl.ANY)] * len(operands),
            out_specs=[pl.BlockSpec(memory_space=pltpu.VMEM)] * 2,
            scratch_shapes=[pltpu.VMEM(x.shape, x.dtype) for x in operands]
            + [
                pltpu.VMEM((n, peers, 1, width), jnp.float32),
                pltpu.VMEM((n * peers, width), jnp.float32),
                pltpu.VMEM((raw, tq.shape[1]), tq.dtype),
                pltpu.VMEM((rank, raw), lq.dtype),
                pltpu.VMEM((SUBLANES, rows - raw if early else rows), jnp.bfloat16),
                pltpu.SemaphoreType.DMA((len(operands),)),
                pltpu.SemaphoreType.DMA((2, n, 3)),
                pltpu.SemaphoreType.DMA((max(1, n - 1), 3)),
                pltpu.SemaphoreType.DMA((2,)),
                pltpu.SemaphoreType.DMA((3,)),
                pltpu.SemaphoreType.DMA((max(1, peers - 1),)),
                pltpu.SemaphoreType.DMA((4,)),
                pltpu.SemaphoreType.DMA((flights,)),
                pltpu.SemaphoreType.DMA((flights,)),
                pltpu.SemaphoreType.REGULAR((1 + 2 * flights,)),
            ],
            compiler_params=pltpu.CompilerParams(collective_id=0, has_side_effects=True),
        )(*operands)
        if whole_tiles:
            *finals, norm = pl.pallas_call(
                functools.partial(settle, places),
                out_shape=[
                    jax.ShapeDtypeStruct((height, n * rows), jnp.bfloat16) for height in heights
                ]
                + [jax.ShapeDtypeStruct(norm.shape, norm.dtype)],
                in_specs=[pl.BlockSpec(memory_space=pltpu.VMEM)] * 2,
                out_specs=[pl.BlockSpec(memory_space=pl.ANY)] * 4,
                scratch_shapes=[pltpu.SemaphoreType.DMA((4,))],
                compiler_params=pltpu.CompilerParams(vmem_limit_bytes=8 * 1024 * 1024),
            )(gathered, norm)
            return (*finals, norm.reshape(-1))
        finals = [
            gathered[:, row : row + height, :].transpose(1, 0, 2).reshape(height, n * rows)
            for row, height in zip(places, heights)
        ]
        return (*finals, norm.reshape(-1))

    in_specs = (
        P(("unit", "rows"), "tp"),
        P(("unit", "rows"), None),
        P("unit", "tp"),
    ) * 3 + (P(("unit", "rows", "tp")),) * 2
    out_specs = (P(("unit", "tp"), None),) * 3 + (P("unit"),)
    return jax.shard_map(shards, mesh=mesh, in_specs=in_specs, out_specs=out_specs, check_vma=False)
```

```python
import functools
import math

import jax
import jax.numpy as jnp
from jax import lax
from jax.experimental import pallas as pl
from jax.experimental.pallas import tpu as pltpu
from jax.sharding import PartitionSpec as P

mix_rate = 0.5
MESH = pl.DeviceIdType.MESH
LANES, SUBLANES = 128, 16
ORDER = (1, 2, 0)


def plan(heights):
    units, row = [], 0
    for which in ORDER:
        height = heights[which]
        width = LANES if height % LANES == 0 else height
        for start in range(0, height, width):
            units.append((which, start, width, row))
            row += width
    edges = [unit[3] for unit in units] + [row]
    cut = sum(unit[0] != ORDER[-1] for unit in units)
    spans = [(0, cut, 0, edges[cut]), (cut, len(units), edges[cut], row - edges[cut])]
    return units, spans, row


def partners(peers, part):
    if peers & (peers - 1):
        return [[(lax.rem(part + step, peers), part, 1) for step in range(1, peers)]]
    rounds, size = [], 1
    while size < peers:
        low = lax.rem(part, 2 * size) < size
        rounds.append([(jnp.where(low, part + size, part - size), part - lax.rem(part, size), size)])
        size *= 2
    return rounds


def kernel(n, peers, rows, early, units, spans, *refs):
    (tq, lq, hq, tk, lk, hk, tv, lv, hv, norm_train, norm_step) = refs[:11]
    gathered, out_norm = refs[11:13]
    held = refs[13:24]
    (gains, sums, raw_train, raw_low, via) = refs[24:29]
    (in_sem, send_sem, recv_sem, extra_send, extra_recv, peer_recv, signs) = refs[29:]
    me, part, unit = lax.axis_index("rows"), lax.axis_index("tp"), lax.axis_index("unit")
    right, left = lax.rem(me + 1, n), lax.rem(me + n - 1, n)
    has_right, has_left = me < n - 1, me > 0
    whole_tiles = len(gathered.shape) == 2
    rounds = partners(peers, part)
    flat = [whom for group in rounds for whom, _, _ in group]
    nearby, told, known = (signs.at[i] for i in range(3))

    barrier = pltpu.get_barrier_semaphore()

    def sign(sem, axis, index):
        pl.semaphore_signal(sem, inc=1, device_id={axis: index}, device_id_type=MESH)

    loads = [
        pltpu.make_async_copy(source, target, in_sem.at[i // 3 if whole_tiles else i])
        for i, (source, target) in enumerate(zip(refs[:11], held))
    ]

    def all_loaded(group):
        if not whole_tiles:
            for load in loads[3 * group : 3 * group + 3]:
                load.wait()
            return
        if group == 3:
            view = gains.at[0, pl.ds(0, 2)]
        else:
            size = sum(math.prod(x.shape) for x in held[3 * group : 3 * group + 3])
            view = gathered.at[pl.ds(0, size // rows), pl.ds(0, rows)]
        pltpu.make_async_copy(view, view, in_sem.at[group]).wait()

    @pl.when(has_right)
    def _():
        sign(barrier, "rows", right)

    @pl.when(me == 0)
    def _():
        for whom in flat:
            sign(barrier, "tp", whom)

    for which in ORDER[:2]:
        for i in (1, 2, 0):
            loads[3 * which + i].start()
    pl.semaphore_wait(barrier, jnp.where(has_left, 1, len(flat)))

    @pl.when(has_left)
    def _():
        sign(nearby, "rows", left)

    def raw_down():
        return pltpu.make_async_remote_copy(
            src_ref=tq.at[pl.ds(0, raw_train.shape[0]), :],
            dst_ref=raw_train,
            send_sem=extra_send.at[0],
            recv_sem=extra_recv.at[0],
            device_id={"rows": left},
            device_id_type=MESH,
        )

    half = raw_low.shape[0] // 2
    carriers = (1, 2)

    def low_down(j):
        return pltpu.make_async_remote_copy(
            src_ref=lq.at[pl.ds(j * half, half), pl.ds(0, LANES)],
            dst_ref=raw_low.at[pl.ds(j * half, half), :],
            send_sem=extra_send.at[1],
            recv_sem=extra_recv.at[1 + j],
            device_id={"rows": left},
            device_id_type=MESH,
        )

    def low_across(j, step):
        return pltpu.make_async_remote_copy(
            src_ref=raw_low.at[pl.ds(j * half, half), :],
            dst_ref=raw_low.at[pl.ds(j * half, half), :],
            send_sem=extra_send.at[step],
            recv_sem=extra_recv.at[1 + j],
            device_id={"tp": lax.rem(carriers[j] + step, peers)},
            device_id_type=MESH,
        )

    def detour(j, leg):
        rows_there = pl.ds(gathered.shape[0] - (2 - j) * SUBLANES, SUBLANES)
        block = gathered.at[rows_there, pl.ds(rows + LANES, rows - LANES)]
        return pltpu.make_async_remote_copy(
            src_ref=(block, via, via)[leg],
            dst_ref=(via, via, block)[leg],
            send_sem=extra_send.at[(1 + j, 2, 0)[leg]],
            recv_sem=extra_recv.at[3 + j],
            device_id=({"tp": carriers[j]}, {"rows": left}, {"tp": 0})[leg],
            device_id_type=MESH,
        )

    if early:

        @pl.when(me == 1)
        def _():
            raw_down().start()

            for j in range(2):

                @pl.when(part == carriers[j])
                def _():
                    low_down(j).start()

    for i in (1, 2, 0, 9, 10):
        loads[i].start()

    FIRST, GAINS, SECOND = range(3)

    def view(c, k, trimmed=0):
        if c == GAINS:
            return gains.at[k]
        _, _, start, height = spans[c // 2]
        if len(gathered.shape) == 3:
            return gathered.at[k, pl.ds(start, height), :]
        skip = LANES if trimmed else 0
        height -= 2 * SUBLANES if trimmed == 2 else 0
        column = pl.multiple_of(k * rows + skip, LANES)
        return gathered.at[pl.ds(start, height), pl.ds(column, rows - skip)]

    def hop(c, k, way, trimmed=0):
        slot = k - 1 if way else k
        return pltpu.make_async_remote_copy(
            src_ref=view(c, k, trimmed),
            dst_ref=view(c, k, trimmed),
            send_sem=send_sem.at[way, c],
            recv_sem=recv_sem.at[slot, c],
            device_id={"rows": left if way else right},
            device_id_type=MESH,
        )

    def send(c, way):
        if not way:

            @pl.when(has_right)
            def _():
                hop(c, me, 0).start()

        elif early and c == SECOND:

            @pl.when((me == 1) & (part == 0))
            def _():
                hop(c, me, 1, 2).start()

            @pl.when((me == 1) & (part > 0))
            def _():
                hop(c, me, 1, 1).start()

            @pl.when(me > 1)
            def _():
                hop(c, me, 1).start()

        else:

            @pl.when(has_left)
            def _():
                hop(c, me, 1).start()

    loaded = set()

    def put(row, width, k, skip, count, high, low, train):
        product = lax.dot_general(
            high, low, (((0,), (0,)), ((), ())), preferred_element_type=jnp.float32
        )
        result = train.T.astype(jnp.float32) + mix_rate * product
        if len(gathered.shape) == 3:
            target = gathered.at[k, pl.ds(row, width), :]
        else:
            column = pl.multiple_of(k * rows + skip, LANES)
            target = gathered.at[pl.ds(row, width), pl.ds(column, count)]
        target[...] = result.astype(jnp.bfloat16)

    def merge(u):
        which, start, width, row = units[u]
        train, low, high = held[3 * which : 3 * which + 3]
        if which not in loaded:
            loaded.add(which)
            all_loaded(which)
        span = pl.ds(start, width)
        put(row, width, me, 0, rows, high[:, span], low[...], train[:, span])

    def merge_span(c):
        for u in range(*spans[c // 2][:2]):
            merge(u)

    merge_span(FIRST)
    send(FIRST, 1)

    @pl.when(has_right)
    def _():
        pl.semaphore_wait(nearby, 1)

    send(FIRST, 0)
    merge_span(SECOND)

    def send_second():
        send(SECOND, 1)
        send(SECOND, 0)

    @pl.when(unit == 0)
    def _():
        send_second()

    all_loaded(3)
    gains[me, part] = held[9][...] + held[10][...]

    @pl.when(has_left)
    def _():
        pl.semaphore_wait(known, 1)

    @pl.when(has_right)
    def _():
        for whom in flat:
            sign(told, "tp", whom)
        pl.semaphore_wait(told, len(flat))
        sign(known, "rows", right)

    flight = 0
    for group in rounds:
        copies = []
        for i, (whom, first, size) in enumerate(group):
            entries = gains.at[me, pl.ds(first, size)]
            copies.append(
                pltpu.make_async_remote_copy(
                    src_ref=entries,
                    dst_ref=entries,
                    send_sem=extra_send.at[3 + i],
                    recv_sem=peer_recv.at[flight],
                    device_id={"tp": whom},
                    device_id_type=MESH,
                )
            )
            flight += 1
        for copy in copies:
            copy.start()
        for copy in copies:
            copy.wait()
    @pl.when(unit != 0)
    def _():
        send_second()

    if early:

        @pl.when(me == 1)
        def _():
            for j in range(2):

                @pl.when(part == 0)
                def _():
                    detour(j, 0).start()

                @pl.when(part == carriers[j])
                def _():
                    detour(j, 0).wait_recv()
                    detour(j, 1).start()

    send(GAINS, 1)
    send(GAINS, 0)

    def take_left(c, step):
        if early and c == SECOND and isinstance(step, int) and step == 1:

            @pl.when((me == 0) & (part == 0))
            def _():
                hop(c, me + step, 1, 2).wait_recv()

            @pl.when((me == 0) & (part > 0))
            def _():
                hop(c, me + step, 1, 1).wait_recv()

            @pl.when(me > 0)
            def _():
                hop(c, me + step, 1).wait_recv()

        else:
            hop(c, me + step, 1).wait_recv()

    def sent_left(c, step):
        if early and c == SECOND and isinstance(step, int) and step == 0:

            @pl.when((me == 1) & (part == 0))
            def _():
                hop(c, me + step, 1, 2).wait_send()

            @pl.when((me == 1) & (part > 0))
            def _():
                hop(c, me + step, 1, 1).wait_send()

            @pl.when(me > 1)
            def _():
                hop(c, me + step, 1).wait_send()

        else:

            @pl.when(has_left)
            def _():
                hop(c, me + step, 1).wait_send()

    def pass_on(step, carry):
        for c in range(3):

            @pl.when(me + step < n)
            def _():
                take_left(c, step)
                sent_left(c, step - 1)

                @pl.when(has_left)
                def _():
                    hop(c, me + step, 1).start()

            @pl.when(me - step >= 0)
            def _():
                hop(c, me - step, 0).wait_recv()

                @pl.when(has_right)
                def _():
                    hop(c, me - step + 1, 0).wait_send()
                    hop(c, me - step, 0).start()

        return carry

    def arrive(c):
        if n > 1:

            @pl.when(me == 0)
            def _():
                take_left(c, n - 1)

            @pl.when(me == n - 1)
            def _():
                hop(c, 0, 0).wait_recv()

    def end_of_line():
        for j in range(2):

            @pl.when(part == carriers[j])
            def _():
                low_down(j).wait_recv()
                for step in range(1, peers):
                    low_across(j, step).start()
                detour(j, 1).wait_recv()
                detour(j, 2).start()

        for j in range(2):

            @pl.when(part != carriers[j])
            def _():
                low_across(j, 1).wait_recv()

        raw_down().wait_recv()
        for which, start, width, row in units:
            if which == 0:
                span = pl.ds(start, width)
                put(row, width, 1, 0, LANES, held[2][:, span], raw_low[...], raw_train[:, span])
        for j in range(2):

            @pl.when(part == 0)
            def _():
                detour(j, 2).wait_recv()

            @pl.when(part == carriers[j])
            def _():
                detour(j, 2).wait_send()
                for step in range(1, peers):
                    low_across(j, step).wait_send()

    if n > 2:
        pass_on(1, 0)
    if early:

        @pl.when(me == 0)
        def _():
            end_of_line()

    if n > 2:
        lax.fori_loop(2, n - 1, pass_on, 0)

    arrive(FIRST)
    arrive(GAINS)
    for k in range(n):
        for t in range(peers):
            sums[k * peers + t : k * peers + t + 1, :] = gains[k, t]
    out_norm[...] = sums[...].astype(jnp.bfloat16)

    if early:

        @pl.when(me == 1)
        def _():
            raw_down().wait_send()
            for j in range(2):

                @pl.when(part == 0)
                def _():
                    detour(j, 0).wait_send()

                @pl.when(part == carriers[j])
                def _():
                    low_down(j).wait_send()
                    detour(j, 1).wait_send()

    for c in range(3):
        if n > 1:

            @pl.when((me == n - 1) & has_left)
            def _():
                hop(c, me, 1).wait_send()

            @pl.when(me == 0)
            def _():
                hop(c, me, 0).wait_send()

        if n > 2:

            @pl.when(has_left & has_right)
            def _():
                hop(c, n - 1, 1).wait_send()
                hop(c, 0, 0).wait_send()

    arrive(SECOND)


def settle(places, gathered, norm, *refs):
    *outs, out_norm, sem = refs
    copies = [
        pltpu.make_async_copy(gathered.at[pl.ds(row, out.shape[0]), :], out, sem.at[i])
        for i, (row, out) in enumerate(zip(places, outs))
    ]
    copies.append(pltpu.make_async_copy(norm, out_norm, sem.at[len(outs)]))
    for copy in copies:
        copy.start()
    for copy in copies:
        copy.wait()


def solution(mesh):
    n, peers = mesh.shape["rows"], mesh.shape["tp"]

    def shards(tq, lq, hq, tk, lk, hk, tv, lv, hv, norm_train, norm_step):
        rows = tq.shape[0]
        whole_tiles = rows % LANES == 0
        operands = (
            tq, lq.T, hq, tk, lk.T, hk, tv, lv.T, hv,
            norm_train.reshape(1, -1), norm_step.reshape(1, -1),
        )
        heights = [train.shape[1] for train in (tq, tk, tv)]
        units, spans, total = plan(heights)
        places = [min(row for which, _, _, row in units if which == i) for i in range(3)]
        width = norm_train.shape[0]
        place = pltpu.VMEM if whole_tiles else jax.ShapeDtypeStruct
        shape = (total, n * rows) if whole_tiles else (n, total, rows)
        rounds = partners(peers, 0)
        flights = max(1, sum(len(group) for group in rounds))
        rank = lq.shape[1]
        early = n > 2 and peers > 2 and whole_tiles and rows > LANES
        early = early and heights[0] % LANES == 0 and rank % (2 * SUBLANES) == 0
        raw = LANES if early else rows
        gathered, norm = pl.pallas_call(
            functools.partial(kernel, n, peers, rows, early, units, spans),
            out_shape=[
                place(shape, jnp.bfloat16),
                place((n * peers, width), jnp.bfloat16),
            ],
            in_specs=[pl.BlockSpec(memory_space=pl.ANY)] * len(operands),
            out_specs=[pl.BlockSpec(memory_space=pltpu.VMEM)] * 2,
            scratch_shapes=[pltpu.VMEM(x.shape, x.dtype) for x in operands]
            + [
                pltpu.VMEM((n, peers, 1, width), jnp.float32),
                pltpu.VMEM((n * peers, width), jnp.float32),
                pltpu.VMEM((raw, tq.shape[1]), tq.dtype),
                pltpu.VMEM((rank, raw), lq.dtype),
                pltpu.VMEM((SUBLANES, rows - raw if early else rows), jnp.bfloat16),
                pltpu.SemaphoreType.DMA((4 if whole_tiles else len(operands),)),
                pltpu.SemaphoreType.DMA((2, 3)),
                pltpu.SemaphoreType.DMA((max(1, n - 1), 3)),
                pltpu.SemaphoreType.DMA((max(4, peers, 3 + max(len(group) for group in rounds)),)),
                pltpu.SemaphoreType.DMA((5,)),
                pltpu.SemaphoreType.DMA((flights,)),
                pltpu.SemaphoreType.REGULAR((3,)),
            ],
            compiler_params=pltpu.CompilerParams(collective_id=0, has_side_effects=True),
        )(*operands)
        if whole_tiles:
            *finals, norm = pl.pallas_call(
                functools.partial(settle, places),
                out_shape=[
                    jax.ShapeDtypeStruct((height, n * rows), jnp.bfloat16) for height in heights
                ]
                + [jax.ShapeDtypeStruct(norm.shape, norm.dtype)],
                in_specs=[pl.BlockSpec(memory_space=pltpu.VMEM)] * 2,
                out_specs=[pl.BlockSpec(memory_space=pl.ANY)] * 4,
                scratch_shapes=[pltpu.SemaphoreType.DMA((4,))],
                compiler_params=pltpu.CompilerParams(vmem_limit_bytes=8 * 1024 * 1024),
            )(gathered, norm)
            return (*finals, norm.reshape(-1))
        finals = [
            gathered[:, row : row + height, :].transpose(1, 0, 2).reshape(height, n * rows)
            for row, height in zip(places, heights)
        ]
        return (*finals, norm.reshape(-1))

    in_specs = (
        P(("unit", "rows"), "tp"),
        P(("unit", "rows"), None),
        P("unit", "tp"),
    ) * 3 + (P(("unit", "rows", "tp")),) * 2
    out_specs = (P(("unit", "tp"), None),) * 3 + (P("unit"),)
    return jax.shard_map(shards, mesh=mesh, in_specs=in_specs, out_specs=out_specs, check_vma=False)
```

```python
import functools
import math

import jax
import jax.numpy as jnp
from jax import lax
from jax.experimental import pallas as pl
from jax.experimental.pallas import tpu as pltpu
from jax.sharding import PartitionSpec as P

mix_rate = 0.5
MESH = pl.DeviceIdType.MESH
LANES, SUBLANES = 128, 16
ORDER = (1, 2, 0)


def plan(heights):
    units, row = [], 0
    for which in ORDER:
        height = heights[which]
        width = LANES if height % LANES == 0 else height
        for start in range(0, height, width):
            units.append((which, start, width, row))
            row += width
    edges = [unit[3] for unit in units] + [row]
    cut = sum(unit[0] != ORDER[-1] for unit in units)
    spans = [(0, cut, 0, edges[cut]), (cut, len(units), edges[cut], row - edges[cut])]
    return units, spans, row


def partners(peers, part):
    if peers & (peers - 1):
        return [[(lax.rem(part + step, peers), part, 1) for step in range(1, peers)]]
    rounds, size = [], 1
    while size < peers:
        low = lax.rem(part, 2 * size) < size
        rounds.append([(jnp.where(low, part + size, part - size), part - lax.rem(part, size), size)])
        size *= 2
    return rounds


def kernel(n, peers, rows, early, units, spans, *refs):
    (tq, lq, hq, tk, lk, hk, tv, lv, hv, norm_train, norm_step) = refs[:11]
    gathered, out_norm = refs[11:13]
    held = refs[13:24]
    (gains, sums, raw_train, raw_low, via) = refs[24:29]
    (in_sem, send_sem, recv_sem, extra_send, extra_recv, peer_recv, signs) = refs[29:]
    me, part, unit = lax.axis_index("rows"), lax.axis_index("tp"), lax.axis_index("unit")
    right, left = lax.rem(me + 1, n), lax.rem(me + n - 1, n)
    has_right, has_left = me < n - 1, me > 0
    whole_tiles = len(gathered.shape) == 2
    rounds = partners(peers, part)
    flat = [whom for group in rounds for whom, _, _ in group]
    nearby, told, known = (signs.at[i] for i in range(3))

    barrier = pltpu.get_barrier_semaphore()

    def sign(sem, axis, index):
        pl.semaphore_signal(sem, inc=1, device_id={axis: index}, device_id_type=MESH)

    loads = [
        pltpu.make_async_copy(source, target, in_sem.at[i // 3 if whole_tiles else i])
        for i, (source, target) in enumerate(zip(refs[:11], held))
    ]

    def all_loaded(group):
        if not whole_tiles:
            for load in loads[3 * group : 3 * group + 3]:
                load.wait()
            return
        if group == 3:
            view = gains.at[0, pl.ds(0, 2)]
        else:
            size = sum(math.prod(x.shape) for x in held[3 * group : 3 * group + 3])
            view = gathered.at[pl.ds(0, size // rows), pl.ds(0, rows)]
        pltpu.make_async_copy(view, view, in_sem.at[group]).wait()

    @pl.when(has_right)
    def _():
        sign(barrier, "rows", right)

    @pl.when(me == 0)
    def _():
        for whom in flat:
            sign(barrier, "tp", whom)

    for which in ORDER[:2]:
        for i in (1, 2, 0):
            loads[3 * which + i].start()
    pl.semaphore_wait(barrier, jnp.where(has_left, 1, len(flat)))

    @pl.when(has_left)
    def _():
        sign(nearby, "rows", left)

    def raw_down():
        return pltpu.make_async_remote_copy(
            src_ref=tq.at[pl.ds(0, raw_train.shape[0]), :],
            dst_ref=raw_train,
            send_sem=extra_send.at[0],
            recv_sem=extra_recv.at[0],
            device_id={"rows": left},
            device_id_type=MESH,
        )

    carriers, low_carrier = (1, 2), peers - 1

    def low_down():
        return pltpu.make_async_remote_copy(
            src_ref=lq.at[:, pl.ds(0, LANES)],
            dst_ref=raw_low,
            send_sem=extra_send.at[1],
            recv_sem=extra_recv.at[1],
            device_id={"rows": left},
            device_id_type=MESH,
        )

    def low_across(step):
        return pltpu.make_async_remote_copy(
            src_ref=raw_low,
            dst_ref=raw_low,
            send_sem=extra_send.at[step],
            recv_sem=extra_recv.at[1],
            device_id={"tp": (low_carrier + step) % peers},
            device_id_type=MESH,
        )

    def detour(j, leg):
        rows_there = pl.ds(gathered.shape[0] - (2 - j) * SUBLANES, SUBLANES)
        block = gathered.at[rows_there, pl.ds(rows + LANES, rows - LANES)]
        return pltpu.make_async_remote_copy(
            src_ref=(block, via, via)[leg],
            dst_ref=(via, via, block)[leg],
            send_sem=extra_send.at[(1 + j, 2, 0)[leg]],
            recv_sem=extra_recv.at[2 + j],
            device_id=({"tp": carriers[j]}, {"rows": left}, {"tp": 0})[leg],
            device_id_type=MESH,
        )

    if early:

        @pl.when(me == 1)
        def _():
            raw_down().start()

            @pl.when(part == low_carrier)
            def _():
                low_down().start()

    for i in (1, 2, 0, 9, 10):
        loads[i].start()

    FIRST, GAINS, SECOND = range(3)

    def view(c, k, trimmed=0):
        if c == GAINS:
            return gains.at[k, part]
        _, _, start, height = spans[c // 2]
        if len(gathered.shape) == 3:
            return gathered.at[k, pl.ds(start, height), :]
        skip = LANES if trimmed else 0
        height -= 2 * SUBLANES if trimmed == 2 else 0
        column = pl.multiple_of(k * rows + skip, LANES)
        return gathered.at[pl.ds(start, height), pl.ds(column, rows - skip)]

    def hop(c, k, way, trimmed=0):
        slot = k - 1 if way else k
        return pltpu.make_async_remote_copy(
            src_ref=view(c, k, trimmed),
            dst_ref=view(c, k, trimmed),
            send_sem=send_sem.at[way, c],
            recv_sem=recv_sem.at[slot, c],
            device_id={"rows": left if way else right},
            device_id_type=MESH,
        )

    def send(c, way):
        if not way:

            @pl.when(has_right)
            def _():
                hop(c, me, 0).start()

        elif early and c == SECOND:

            @pl.when((me == 1) & (part == 0))
            def _():
                hop(c, me, 1, 2).start()

            @pl.when((me == 1) & (part > 0))
            def _():
                hop(c, me, 1, 1).start()

            @pl.when(me > 1)
            def _():
                hop(c, me, 1).start()

        else:

            @pl.when(has_left)
            def _():
                hop(c, me, 1).start()

    loaded = set()

    def put(row, width, k, skip, count, high, low, train):
        product = lax.dot_general(
            high, low, (((0,), (0,)), ((), ())), preferred_element_type=jnp.float32
        )
        result = train.T.astype(jnp.float32) + mix_rate * product
        if len(gathered.shape) == 3:
            target = gathered.at[k, pl.ds(row, width), :]
        else:
            column = pl.multiple_of(k * rows + skip, LANES)
            target = gathered.at[pl.ds(row, width), pl.ds(column, count)]
        target[...] = result.astype(jnp.bfloat16)

    def merge(u):
        which, start, width, row = units[u]
        train, low, high = held[3 * which : 3 * which + 3]
        if which not in loaded:
            loaded.add(which)
            all_loaded(which)
        span = pl.ds(start, width)
        put(row, width, me, 0, rows, high[:, span], low[...], train[:, span])

    def merge_span(c):
        for u in range(*spans[c // 2][:2]):
            merge(u)

    yields = (unit > 0) & (me == 1) if early else me < 0
    merge_span(FIRST)

    @pl.when(~yields)
    def _():
        send(FIRST, 1)

    @pl.when(has_right)
    def _():
        pl.semaphore_wait(nearby, 1)

    send(FIRST, 0)
    all_loaded(3)
    gains[me, part] = held[9][...] + held[10][...]
    merge_span(SECOND)

    @pl.when(~yields)
    def _():
        send(GAINS, 1)

    send(GAINS, 0)

    def send_second():
        send(SECOND, 1)
        send(SECOND, 0)

    @pl.when(unit == 0)
    def _():
        send_second()

    @pl.when(has_left)
    def _():
        pl.semaphore_wait(known, 1)

    @pl.when(has_right)
    def _():
        for whom in flat:
            sign(told, "tp", whom)
        pl.semaphore_wait(told, len(flat))
        sign(known, "rows", right)

    @pl.when(yields)
    def _():
        send(FIRST, 1)
        send(GAINS, 1)

    if early:

        @pl.when(me == 1)
        def _():
            for j in range(2):

                @pl.when(part == 0)
                def _():
                    detour(j, 0).start()

                @pl.when(part == carriers[j])
                def _():
                    detour(j, 0).wait_recv()
                    detour(j, 1).start()

    def take_left(c, step):
        if early and c == SECOND and isinstance(step, int) and step == 1:

            @pl.when((me == 0) & (part == 0))
            def _():
                hop(c, me + step, 1, 2).wait_recv()

            @pl.when((me == 0) & (part > 0))
            def _():
                hop(c, me + step, 1, 1).wait_recv()

            @pl.when(me > 0)
            def _():
                hop(c, me + step, 1).wait_recv()

        else:
            hop(c, me + step, 1).wait_recv()

    def sent_left(c, step):
        if early and c == SECOND and isinstance(step, int) and step == 0:

            @pl.when((me == 1) & (part == 0))
            def _():
                hop(c, me + step, 1, 2).wait_send()

            @pl.when((me == 1) & (part > 0))
            def _():
                hop(c, me + step, 1, 1).wait_send()

            @pl.when(me > 1)
            def _():
                hop(c, me + step, 1).wait_send()

        else:

            @pl.when(has_left)
            def _():
                hop(c, me + step, 1).wait_send()

    def pass_on(step, carry):
        for c in range(3):

            @pl.when(me + step < n)
            def _():
                take_left(c, step)
                sent_left(c, step - 1)

                @pl.when(has_left)
                def _():
                    hop(c, me + step, 1).start()

            @pl.when(me - step >= 0)
            def _():
                hop(c, me - step, 0).wait_recv()

                @pl.when(has_right)
                def _():
                    hop(c, me - step + 1, 0).wait_send()
                    hop(c, me - step, 0).start()

            if isinstance(step, int) and c == FIRST:

                @pl.when(unit > 0)
                def _():
                    send_second()

        return carry

    def arrive(c):
        if n > 1:

            @pl.when(me == 0)
            def _():
                take_left(c, n - 1)

            @pl.when(me == n - 1)
            def _():
                hop(c, 0, 0).wait_recv()

    def end_of_line():
        @pl.when(part == low_carrier)
        def _():
            low_down().wait_recv()
            for step in range(1, peers):
                low_across(step).start()

        for j in range(2):

            @pl.when(part == carriers[j])
            def _():
                detour(j, 1).wait_recv()
                detour(j, 2).start()

        @pl.when(part != low_carrier)
        def _():
            low_across(1).wait_recv()

        raw_down().wait_recv()
        for which, start, width, row in units:
            if which == 0:
                span = pl.ds(start, width)
                put(row, width, 1, 0, LANES, held[2][:, span], raw_low[...], raw_train[:, span])
        for j in range(2):

            @pl.when(part == 0)
            def _():
                detour(j, 2).wait_recv()

            @pl.when(part == carriers[j])
            def _():
                detour(j, 2).wait_send()

        @pl.when(part == low_carrier)
        def _():
            for step in range(1, peers):
                low_across(step).wait_send()

    if n > 2:
        pass_on(1, 0)
    else:

        @pl.when(unit > 0)
        def _():
            send_second()

    if early:

        @pl.when(me == 0)
        def _():
            end_of_line()

    if n > 2:
        lax.fori_loop(2, n - 1, pass_on, 0)

    arrive(FIRST)
    arrive(GAINS)

    flight = 0
    for group in rounds:
        copies = []
        for i, (whom, first, size) in enumerate(group):
            entries = gains.at[:, pl.ds(first, size)]
            copies.append(
                pltpu.make_async_remote_copy(
                    src_ref=entries,
                    dst_ref=entries,
                    send_sem=extra_send.at[3 + i],
                    recv_sem=peer_recv.at[flight],
                    device_id={"tp": whom},
                    device_id_type=MESH,
                )
            )
            flight += 1
        for copy in copies:
            copy.start()
        for copy in copies:
            copy.wait()
    for k in range(n):
        for t in range(peers):
            sums[k * peers + t : k * peers + t + 1, :] = gains[k, t]
    out_norm[...] = sums[...].astype(jnp.bfloat16)

    if early:

        @pl.when(me == 1)
        def _():
            raw_down().wait_send()
            for j in range(2):

                @pl.when(part == 0)
                def _():
                    detour(j, 0).wait_send()

                @pl.when(part == carriers[j])
                def _():
                    detour(j, 1).wait_send()

            @pl.when(part == low_carrier)
            def _():
                low_down().wait_send()

    for c in range(3):
        if n > 1:

            @pl.when((me == n - 1) & has_left)
            def _():
                hop(c, me, 1).wait_send()

            @pl.when(me == 0)
            def _():
                hop(c, me, 0).wait_send()

        if n > 2:

            @pl.when(has_left & has_right)
            def _():
                hop(c, n - 1, 1).wait_send()
                hop(c, 0, 0).wait_send()

    arrive(SECOND)


def settle(places, gathered, norm, *refs):
    *outs, out_norm, sem = refs
    copies = [
        pltpu.make_async_copy(gathered.at[pl.ds(row, out.shape[0]), :], out, sem.at[i])
        for i, (row, out) in enumerate(zip(places, outs))
    ]
    copies.append(pltpu.make_async_copy(norm, out_norm, sem.at[len(outs)]))
    for copy in copies:
        copy.start()
    for copy in copies:
        copy.wait()


def solution(mesh):
    n, peers = mesh.shape["rows"], mesh.shape["tp"]

    def shards(tq, lq, hq, tk, lk, hk, tv, lv, hv, norm_train, norm_step):
        rows = tq.shape[0]
        whole_tiles = rows % LANES == 0
        operands = (
            tq, lq.T, hq, tk, lk.T, hk, tv, lv.T, hv,
            norm_train.reshape(1, -1), norm_step.reshape(1, -1),
        )
        heights = [train.shape[1] for train in (tq, tk, tv)]
        units, spans, total = plan(heights)
        places = [min(row for which, _, _, row in units if which == i) for i in range(3)]
        width = norm_train.shape[0]
        place = pltpu.VMEM if whole_tiles else jax.ShapeDtypeStruct
        shape = (total, n * rows) if whole_tiles else (n, total, rows)
        rounds = partners(peers, 0)
        flights = max(1, sum(len(group) for group in rounds))
        rank = lq.shape[1]
        early = n > 2 and peers > 3 and whole_tiles and rows > LANES
        early = early and heights[0] % LANES == 0
        raw = LANES if early else rows
        gathered, norm = pl.pallas_call(
            functools.partial(kernel, n, peers, rows, early, units, spans),
            out_shape=[
                place(shape, jnp.bfloat16),
                place((n * peers, width), jnp.bfloat16),
            ],
            in_specs=[pl.BlockSpec(memory_space=pl.ANY)] * len(operands),
            out_specs=[pl.BlockSpec(memory_space=pltpu.VMEM)] * 2,
            scratch_shapes=[pltpu.VMEM(x.shape, x.dtype) for x in operands]
            + [
                pltpu.VMEM((n, peers, 1, width), jnp.float32),
                pltpu.VMEM((n * peers, width), jnp.float32),
                pltpu.VMEM((raw, tq.shape[1]), tq.dtype),
                pltpu.VMEM((rank, raw), lq.dtype),
                pltpu.VMEM((SUBLANES, rows - raw if early else rows), jnp.bfloat16),
                pltpu.SemaphoreType.DMA((4 if whole_tiles else len(operands),)),
                pltpu.SemaphoreType.DMA((2, 3)),
                pltpu.SemaphoreType.DMA((max(1, n - 1), 3)),
                pltpu.SemaphoreType.DMA((max(4, peers, 3 + max(len(group) for group in rounds)),)),
                pltpu.SemaphoreType.DMA((4,)),
                pltpu.SemaphoreType.DMA((flights,)),
                pltpu.SemaphoreType.REGULAR((3,)),
            ],
            compiler_params=pltpu.CompilerParams(collective_id=0, has_side_effects=True),
        )(*operands)
        if whole_tiles:
            *finals, norm = pl.pallas_call(
                functools.partial(settle, places),
                out_shape=[
                    jax.ShapeDtypeStruct((height, n * rows), jnp.bfloat16) for height in heights
                ]
                + [jax.ShapeDtypeStruct(norm.shape, norm.dtype)],
                in_specs=[pl.BlockSpec(memory_space=pltpu.VMEM)] * 2,
                out_specs=[pl.BlockSpec(memory_space=pl.ANY)] * 4,
                scratch_shapes=[pltpu.SemaphoreType.DMA((4,))],
                compiler_params=pltpu.CompilerParams(vmem_limit_bytes=8 * 1024 * 1024),
            )(gathered, norm)
            return (*finals, norm.reshape(-1))
        finals = [
            gathered[:, row : row + height, :].transpose(1, 0, 2).reshape(height, n * rows)
            for row, height in zip(places, heights)
        ]
        return (*finals, norm.reshape(-1))

    in_specs = (
        P(("unit", "rows"), "tp"),
        P(("unit", "rows"), None),
        P("unit", "tp"),
    ) * 3 + (P(("unit", "rows", "tp")),) * 2
    out_specs = (P(("unit", "tp"), None),) * 3 + (P("unit"),)
    return jax.shard_map(shards, mesh=mesh, in_specs=in_specs, out_specs=out_specs, check_vma=False)
```
